16 devices in a mesh: dp: 2 (over y, z), ep: 8 (over x, core).
Axes of the slice: x: 4, y: 2, z: 1, core: 2. Of those that a mesh axis runs over, the one named last changes fastest.
The devices are a block of a 4x4x8 slice.
Arguments:
- tokens: bfloat16 [1024, 2048], P(('dp', 'ep')), parts along dimension 0
- route_idx: int32 [1024, 8], P(('dp', 'ep')), parts along dimension 0
- gate_vals: float32 [1024, 8], P(('dp', 'ep')), parts along dimension 0
- w_gate: bfloat16 [64, 2048, 1024], P('ep')
- w_up: bfloat16 [64, 2048, 1024], P('ep')
- w_down: bfloat16 [64, 1024, 2048], P('ep')
Outputs:
- output: bfloat16 [1024, 2048], P(('dp', 'ep')), parts along dimension 0
There are 2 independent parts. The reference program is written for one: setup_inputs(seed, part) draws one part's arguments, and reference() takes and returns one part's arrays. A program takes and returns all parts, laid end to end along the dimension named above; an argument that names none is the same for every part.
All inputs are finite; a program needn't handle non-finite values.
Results may differ from the reference program's by a relative error of at most 0.00782637.
Values are sent between devices in bfloat16 or wider.
A program may use at most 768 MiB of HBM per device.

```python
import functools
import jax
import jax.numpy as jnp
from jax import lax

TOKENS_DEV = 64
GROUP_SIZE = 8
D_MODEL = 2048
D_FF = 1024
EXPERTS = 64
TOP_K = 8
CAPACITY = 32
TOKENS = TOKENS_DEV * GROUP_SIZE


def device_routing(expert_order, hot_counts, dev_key):
    key_jitter, key_perm, key_tokens = jax.random.split(dev_key, 3)
    cold_n = EXPERTS - TOP_K
    half_n = cold_n // 2
    rest_slots = TOKENS_DEV * TOP_K - jnp.sum(hot_counts)
    base_count = rest_slots // cold_n
    extra_count = rest_slots - base_count * cold_n
    cold_counts = base_count + (jnp.arange(cold_n) < extra_count).astype(jnp.int32)
    jitter_up = jax.random.randint(key_jitter, (half_n,), 0, (base_count - 1) // 2 + 1)
    jitter = jnp.stack([jitter_up, -jitter_up], axis=1).reshape(-1)
    jitter = jnp.pad(jitter, (0, cold_n - 2 * half_n))
    cold_counts = cold_counts + jax.random.permutation(key_perm, jitter)
    all_counts = jnp.concatenate([hot_counts, cold_counts])
    run_ends = jnp.cumsum(all_counts)
    rank_ids = jnp.searchsorted(run_ends, jnp.arange(TOKENS_DEV * TOP_K), side="right")
    flat_ids = expert_order[rank_ids]
    slot_grid = flat_ids.reshape(TOP_K, TOKENS_DEV).T
    return jax.random.permutation(key_tokens, slot_grid, axis=0)


def draw_routing(route_key):
    key_order, key_hot, key_pick, key_dev = jax.random.split(route_key, 4)
    expert_order = jax.random.permutation(key_order, EXPERTS)
    hot_counts = CAPACITY - jax.random.randint(key_hot, (GROUP_SIZE, TOP_K), 0, CAPACITY // 4 + 1)
    full_dev = jax.random.randint(key_pick, (), 0, GROUP_SIZE)
    at_full = (jnp.arange(GROUP_SIZE)[:, None] == full_dev) & (jnp.arange(TOP_K)[None, :] == 0)
    hot_counts = jnp.where(at_full, CAPACITY, hot_counts)
    dev_keys = jax.random.split(key_dev, GROUP_SIZE)
    per_device = jax.vmap(functools.partial(device_routing, expert_order))(hot_counts, dev_keys)
    return per_device.reshape(TOKENS, TOP_K).astype(jnp.int32)


def draw_weight(weight_key, fan_in, fan_out):
    expert_keys = jax.random.split(weight_key, EXPERTS)
    return lax.map(lambda one_key: (jax.random.normal(one_key, (fan_in, fan_out), jnp.float32) * fan_in ** -0.5).astype(jnp.bfloat16), expert_keys)


def setup_inputs(seed: int = 0, part: int = 0) -> dict:
    root_key = jax.random.key(seed)
    part_key = jax.random.fold_in(root_key, part)
    key_tok, key_route, key_gate = jax.random.split(part_key, 3)
    key_wg, key_wu, key_wd = jax.random.split(jax.random.key(seed + 1), 3)
    tokens = jax.random.normal(key_tok, (TOKENS, D_MODEL), jnp.float32).astype(jnp.bfloat16)
    route_idx = draw_routing(key_route)
    gate_vals = jax.random.uniform(key_gate, (TOKENS, TOP_K), jnp.float32, 0.5, 1.5) * TOP_K ** -0.5
    return {"tokens": tokens, "route_idx": route_idx, "gate_vals": gate_vals, "w_gate": draw_weight(key_wg, D_MODEL, D_FF), "w_up": draw_weight(key_wu, D_MODEL, D_FF), "w_down": draw_weight(key_wd, D_FF, D_MODEL)}


def reference(tokens, route_idx, gate_vals, w_gate, w_up, w_down):
    row_cap = GROUP_SIZE * CAPACITY
    targets = jnp.arange(row_cap) + 1

    def expert_step(y_acc, expert_args):
        expert_id, wg_one, wu_one, wd_one = expert_args
        hit_mask = route_idx == expert_id
        member = jnp.sum(hit_mask, axis=1, dtype=jnp.int32)
        row_weight = jnp.sum(jnp.where(hit_mask, gate_vals, 0.0), axis=1)
        row_ids = jnp.searchsorted(jnp.cumsum(member), targets, side="left")
        picked = jnp.take(tokens, row_ids, axis=0, mode="fill", fill_value=0)
        pre_gate = jnp.dot(picked, wg_one, preferred_element_type=jnp.float32)
        pre_up = jnp.dot(picked, wu_one, preferred_element_type=jnp.float32)
        hidden = (jax.nn.silu(pre_gate) * pre_up).astype(jnp.bfloat16)
        expert_out = jnp.dot(hidden, wd_one, preferred_element_type=jnp.float32).astype(jnp.bfloat16)
        row_gate = jnp.take(row_weight, row_ids, mode="fill", fill_value=0.0)
        y_acc = y_acc.at[row_ids].add(row_gate[:, None] * expert_out.astype(jnp.float32), mode="drop")
        return y_acc, None

    y_init = jnp.zeros((TOKENS, D_MODEL), jnp.float32)
    y_sum, unused = lax.scan(expert_step, y_init, (jnp.arange(EXPERTS), w_gate, w_up, w_down))
    return y_sum.astype(jnp.bfloat16)
```

```python
import functools

import jax
import jax.numpy as jnp
from jax import lax
from jax.experimental import pallas as pl
from jax.experimental.pallas import tpu as pltpu
from jax.sharding import PartitionSpec as P

F32 = jnp.float32
BF16 = jnp.bfloat16
KCHUNKS = 4
COLS = 256
WSLOTS = 8
DSLOTS = 2


def moe_kernel(dims, x_hbm, comb_in, wg_hbm, wu_hbm, wd_hbm, y_ref,
               xbuf, comb, codes, pmat, smat, gmat, gacc, uacc, hid, wgb, wub, wdb, acc, sib, red, ra, rb, rl, rr,
               x_sem, comb_send, comb_recv, ag_send, ag_recv, w_sem, d_sem, rs_send, rs_recv):
    n, tok_dev, d_model, d_ff, n_exp, top_k, cap = dims
    chips = n // 2
    kw = d_model // KCHUNKS
    n_items = KCHUNKS * n_exp
    n_chunks = d_model // COLS
    half_tok = n * tok_dev // 2
    half_slot = n * cap // 2

    me = lax.axis_index("ep")
    chip, core = me // 2, me % 2
    sibling = chip * 2 + (1 - core)
    c_right, c_left, c_opp = (chip + 1) % chips, (chip + chips - 1) % chips, (chip + 2) % chips
    right, left, opp = c_right * 2 + core, c_left * 2 + core, c_opp * 2 + core
    other = 1 - core

    def remote(src, dst, send, recv, dev):
        return pltpu.make_async_remote_copy(src_ref=src, dst_ref=dst, send_sem=send, recv_sem=recv,
                                            device_id={"ep": dev}, device_id_type=pl.DeviceIdType.MESH)

    def x_copy(kc):
        return pltpu.make_async_copy(x_hbm.at[:, pl.ds(kc * kw, kw)],
                                     xbuf.at[kc, pl.ds(pl.multiple_of(me * tok_dev, tok_dev), tok_dev), :], x_sem.at[kc])

    def w_copies(item):
        e, kc, slot = item % n_exp, item // n_exp, item % WSLOTS
        rows = pl.ds(pl.multiple_of(kc * kw, kw), kw)
        return (pltpu.make_async_copy(wg_hbm.at[e, rows, :], wgb.at[slot], w_sem.at[slot, 0]),
                pltpu.make_async_copy(wu_hbm.at[e, rows, :], wub.at[slot], w_sem.at[slot, 1]))

    def d_copy(c):
        slot = c % DSLOTS
        return pltpu.make_async_copy(wd_hbm.at[:, :, pl.ds(pl.multiple_of(c * COLS, COLS), COLS)], wdb.at[slot], d_sem.at[slot])

    for kc in range(KCHUNKS):
        x_copy(kc).start()
    for item in range(WSLOTS):
        for copy in w_copies(item):
            copy.start()

    barrier = pltpu.get_barrier_semaphore()
    for off in range(1, n):
        pl.semaphore_signal(barrier, inc=1, device_id={"ep": (me + off) % n}, device_id_type=pl.DeviceIdType.MESH)
    pl.semaphore_wait(barrier, n - 1)

    def block(kc, src):
        return xbuf.at[kc, pl.ds(pl.multiple_of(src * tok_dev, tok_dev), tok_dev), :]

    def ag_copy(kc, src, lane, dev):
        return remote(block(kc, src), block(kc, src), ag_send.at[kc, lane], ag_recv.at[kc, src], dev)

    def send_own(kc):
        x_copy(kc).wait()
        ag_copy(kc, me, 0, right).start()
        ag_copy(kc, me, 1, left).start()
        ag_copy(kc, me, 2, sibling).start()

    def relay_near(kc):
        ag_copy(kc, left, 3, sibling).wait_recv()
        ag_copy(kc, right, 4, sibling).wait_recv()
        if kc % 2 == 0:
            ag_copy(kc, left, 5, right).start()
        else:
            ag_copy(kc, right, 5, left).start()
        ag_copy(kc, left, 3, sibling).start()
        ag_copy(kc, right, 4, sibling).start()

    def relay_far(kc):
        ag_copy(kc, opp, 6, sibling).wait_recv()
        ag_copy(kc, opp, 6, sibling).start()

    def gathered(kc):
        for c in (chip, c_left, c_right, c_opp):
            ag_copy(kc, c * 2 + other, 2, sibling).wait_recv()

    send_own(0)
    comb_copies = []
    for off in range(1, n):
        copy = remote(comb_in, comb.at[me], comb_send.at[off - 1], comb_recv.at[me], (me + off) % n)
        copy.start()
        comb_copies.append(copy)
    comb[me] = comb_in[...]
    send_own(1)

    acc[...] = jnp.zeros_like(acc)

    for off in range(1, n):
        src = (me + off) % n
        remote(comb_in, comb.at[src], comb_send.at[off - 1], comb_recv.at[src], src).wait_recv()

    lanes = 2 * tok_dev
    t_row = lax.broadcasted_iota(jnp.int32, (lanes, lanes), 0)
    t_col = lax.broadcasted_iota(jnp.int32, (lanes, lanes), 1)
    before = jnp.where((t_row < t_col) & (t_row // tok_dev == t_col // tok_dev), 1.0, 0.0).astype(BF16)
    e_id = (lax.broadcasted_iota(jnp.int32, (n_exp, lanes), 0) + me * n_exp).astype(F32)
    lane_base = ((lax.broadcasted_iota(jnp.int32, (n_exp, lanes), 1) // tok_dev) * cap).astype(F32)
    for c in range(chips):
        both = comb[2 * c] + comb[2 * c + 1]
        hits = jnp.zeros((n_exp, lanes), F32)
        gates = jnp.zeros((n_exp, lanes), F32)
        for k in range(top_k):
            same = jnp.broadcast_to(both[k:k + 1, :], (n_exp, lanes)) == e_id
            hits = hits + jnp.where(same, 1.0, 0.0)
            gates = gates + jnp.where(same, jnp.broadcast_to(both[top_k + k:top_k + k + 1, :], (n_exp, lanes)), 0.0)
        rank = jnp.dot(hits.astype(BF16), before, preferred_element_type=F32)
        code = jnp.where(hits > 0.0, rank + lane_base + float((c % 2) * 2 * cap), -1.0)
        codes[c, 0:n_exp, :] = code
        codes[c, n_exp:2 * n_exp, :] = gates

    def tables(e, carry):
        slot_row = lax.broadcasted_iota(jnp.int32, (half_slot, lanes), 0).astype(F32)
        slot_col = lax.broadcasted_iota(jnp.int32, (lanes, half_slot), 1).astype(F32)
        for c in range(chips):
            code = jnp.broadcast_to(codes[c, pl.ds(e, 1), :], (half_slot, lanes))
            pmat[e, c // 2, :, (c % 2) * lanes:(c % 2 + 1) * lanes] = jnp.where(code == slot_row, 1.0, 0.0).astype(BF16)
            smat[e, c // 2, (c % 2) * lanes:(c % 2 + 1) * lanes, :] = jnp.where(code.T == slot_col, 1.0, 0.0).astype(BF16)
            gate = jnp.broadcast_to(codes[c, pl.ds(n_exp + e, 1), :], (lanes, lanes))
            gmat[e, c * lanes:(c + 1) * lanes, :] = gate.T
        return carry

    relay_near(0)
    send_own(2)
    lax.fori_loop(0, n_exp, tables, 0)
    relay_far(0)
    gathered(0)

    def expert_chunk(kc, e):
        item = kc * n_exp + e
        slot = item % WSLOTS
        for copy in w_copies(item):
            copy.wait()
        rows = [jnp.dot(pmat[e, h], xbuf[kc, h * half_tok:(h + 1) * half_tok, :], preferred_element_type=F32) for h in range(2)]
        xs = jnp.concatenate(rows, axis=0).astype(BF16)
        for c in range(d_ff // 256):
            cols = slice(c * 256, (c + 1) * 256)
            g = jnp.dot(xs, wgb[slot, :, cols], preferred_element_type=F32)
            u = jnp.dot(xs, wub[slot, :, cols], preferred_element_type=F32)
            if kc > 0:
                g = gacc[e, :, cols] + g
                u = uacc[e, :, cols] + u
            if kc < KCHUNKS - 1:
                gacc[e, :, cols] = g
                uacc[e, :, cols] = u
            else:
                hid[e, :, cols] = (jax.nn.silu(g) * u).astype(BF16)

        @pl.when(item + WSLOTS < n_items)
        def _():
            for copy in w_copies(item + WSLOTS):
                copy.start()

    for kc in range(KCHUNKS):
        def body(e, carry, kc=kc):
            expert_chunk(kc, e)
            nxt = kc + 1
            if nxt < KCHUNKS:
                @pl.when(e == 1)
                def _():
                    relay_near(nxt)
                    if nxt + 2 < KCHUNKS:
                        send_own(nxt + 2)

                @pl.when(e == n_exp - 3)
                def _():
                    relay_far(nxt)
            else:
                @pl.when(e < DSLOTS)
                def _():
                    d_copy(e).start()
            return carry

        lax.fori_loop(0, n_exp, body, 0)
        if kc + 1 < KCHUNKS:
            gathered(kc + 1)

    def to_sibling(c):
        return remote(acc.at[c, :, other], sib.at[c], rs_send.at[0, c], rs_recv.at[0, c], sibling)

    def far_right(c):
        return remote(red.at[c, c_opp, :, pl.ds(0, COLS // 2)], ra.at[c], rs_send.at[1, c], rs_recv.at[1, c], right)

    def far_left(c):
        return remote(red.at[c, c_opp, :, pl.ds(COLS // 2, COLS // 2)], rb.at[c], rs_send.at[2, c], rs_recv.at[2, c], left)

    def near_right(c):
        return remote(red.at[c, c_right], rl.at[c], rs_send.at[3, c], rs_recv.at[3, c], right)

    def near_left(c):
        return remote(red.at[c, c_left], rr.at[c], rs_send.at[4, c], rs_recv.at[4, c], left)

    def stage2(c):
        to_sibling(c).wait_recv()
        red[c] = acc[c, :, core] + sib[c]
        far_right(c).start()
        far_left(c).start()

    def stage3(c):
        far_right(c).wait_recv()
        red[c, c_right, :, :COLS // 2] = red[c, c_right, :, :COLS // 2] + ra[c]
        near_right(c).start()
        far_left(c).wait_recv()
        red[c, c_left, :, COLS // 2:] = red[c, c_left, :, COLS // 2:] + rb[c]
        near_left(c).start()

    def stage4(c):
        near_right(c).wait_recv()
        near_left(c).wait_recv()
        y_ref[:, pl.ds(pl.multiple_of(c * COLS, COLS), COLS)] = (red[c, chip] + rl[c] + rr[c]).astype(BF16)

    def down(c):
        slot = c % DSLOTS
        d_copy(c).wait()
        for e in range(n_exp):
            out = jnp.dot(hid[e], wdb[slot, e], preferred_element_type=F32).astype(BF16)
            for ch in range(chips):
                h, rows = ch // 2, slice((ch % 2) * lanes, (ch % 2 + 1) * lanes)
                put = jnp.dot(smat[e, h, rows, :], out[h * half_slot:(h + 1) * half_slot], preferred_element_type=F32)
                gate = gmat[e, ch * lanes:(ch + 1) * lanes, :]
                put = put * jnp.concatenate([gate] * (COLS // lanes), axis=1)
                acc[c, ch] = acc[c, ch] + put.reshape(2, tok_dev, COLS)

        @pl.when(c + DSLOTS < n_chunks)
        def _():
            d_copy(c + DSLOTS).start()

    def chunk_body(c, carry):
        down(c)
        to_sibling(c).start()

        @pl.when(c >= 1)
        def _():
            stage2(c - 1)

        @pl.when(c >= 2)
        def _():
            stage3(c - 2)

        @pl.when(c >= 3)
        def _():
            stage4(c - 3)
        return carry

    lax.fori_loop(0, n_chunks, chunk_body, 0)
    last = n_chunks - 1
    stage2(last)
    stage3(last - 1)
    stage4(last - 2)
    stage3(last)
    stage4(last - 1)
    stage4(last)

    for copy in comb_copies:
        copy.wait_send()
    for kc in range(KCHUNKS):
        for lane, (src, dev) in enumerate(((me, right), (me, left), (me, sibling), (left, sibling), (right, sibling),
                                           (left, right) if kc % 2 == 0 else (right, left), (opp, sibling))):
            ag_copy(kc, src, lane, dev).wait_send()

    def drain(c, carry):
        for make in (to_sibling, far_right, far_left, near_right, near_left):
            make(c).wait_send()
        return carry

    lax.fori_loop(0, n_chunks, drain, 0)


def solution(mesh):
    n = mesh.shape["ep"]
    row_spec = P(("dp", "ep"))
    expert_spec = P("ep")

    def local_step(tok, route, gate, wg, wu, wd):
        tok_dev, d_model = tok.shape
        n_exp, _, d_ff = wg.shape
        top_k = route.shape[1]
        cap = tok_dev // 2
        chips = n // 2
        lanes = 2 * tok_dev
        kw = d_model // KCHUNKS
        n_chunks = d_model // COLS
        dims = (n, tok_dev, d_model, d_ff, n_exp, top_k, cap)

        table = jnp.concatenate([route.astype(F32).T, gate.T], axis=0)
        mine = lax.broadcasted_iota(jnp.int32, (1, lanes), 1) // tok_dev == lax.axis_index("ep") % 2
        empty = jnp.where(lax.broadcasted_iota(jnp.int32, (2 * top_k, 1), 0) < top_k, 0.0, 0.0)
        table = jnp.where(mine, jnp.concatenate([table, table], axis=1), empty)

        hbm = pl.BlockSpec(memory_space=pl.ANY)
        vmem = pl.BlockSpec(memory_space=pltpu.VMEM)
        return pl.pallas_call(
            functools.partial(moe_kernel, dims),
            out_shape=jax.ShapeDtypeStruct((tok_dev, d_model), BF16),
            in_specs=[hbm, vmem, hbm, hbm, hbm],
            out_specs=vmem,
            scratch_shapes=[
                pltpu.VMEM((KCHUNKS, n * tok_dev, kw), BF16),
                pltpu.VMEM((n, 2 * top_k, lanes), F32),
                pltpu.VMEM((chips, 2 * n_exp, lanes), F32),
                pltpu.VMEM((n_exp, 2, n * cap // 2, n * tok_dev // 2), BF16),
                pltpu.VMEM((n_exp, 2, n * tok_dev // 2, n * cap // 2), BF16),
                pltpu.VMEM((n_exp, n * tok_dev, lanes), F32),
                pltpu.VMEM((n_exp, n * cap, d_ff), F32),
                pltpu.VMEM((n_exp, n * cap, d_ff), F32),
                pltpu.VMEM((n_exp, n * cap, d_ff), BF16),
                pltpu.VMEM((WSLOTS, kw, d_ff), BF16),
                pltpu.VMEM((WSLOTS, kw, d_ff), BF16),
                pltpu.VMEM((DSLOTS, n_exp, d_ff, COLS), BF16),
                pltpu.VMEM((n_chunks, chips, 2, tok_dev, COLS), F32),
                pltpu.VMEM((n_chunks, chips, tok_dev, COLS), F32),
                pltpu.VMEM((n_chunks, chips, tok_dev, COLS), F32),
                pltpu.VMEM((n_chunks, tok_dev, COLS // 2), F32),
                pltpu.VMEM((n_chunks, tok_dev, COLS // 2), F32),
                pltpu.VMEM((n_chunks, tok_dev, COLS), F32),
                pltpu.VMEM((n_chunks, tok_dev, COLS), F32),
                pltpu.SemaphoreType.DMA((KCHUNKS,)),
                pltpu.SemaphoreType.DMA((n - 1,)),
                pltpu.SemaphoreType.DMA((n,)),
                pltpu.SemaphoreType.DMA((KCHUNKS, 7)),
                pltpu.SemaphoreType.DMA((KCHUNKS, n)),
                pltpu.SemaphoreType.DMA((WSLOTS, 2)),
                pltpu.SemaphoreType.DMA((DSLOTS,)),
                pltpu.SemaphoreType.DMA((5, n_chunks)),
                pltpu.SemaphoreType.DMA((5, n_chunks)),
            ],
            compiler_params=pltpu.CompilerParams(collective_id=0, has_side_effects=True, vmem_limit_bytes=67_043_328),
        )(tok, table, wg, wu, wd)

    return jax.shard_map(local_step, mesh=mesh, in_specs=(row_spec, row_spec, row_spec, expert_spec, expert_spec, expert_spec), out_specs=row_spec, check_vma=False)
```

```python
import functools

import jax
import jax.numpy as jnp
from jax import lax
from jax.experimental import pallas as pl
from jax.experimental.pallas import tpu as pltpu
from jax.sharding import PartitionSpec as P

F32 = jnp.float32
BF16 = jnp.bfloat16
KCHUNKS = 4
COLS = 256
SLOTS = 26


def moe_kernel(dims, x_hbm, route_ref, gate_ref, wg_hbm, wu_hbm, wd_hbm, y_ref,
               xbuf, table, comb_in, comb, codes, pmat, smat, gmat, gacc, uacc, hid, ring, outs, acc, sib, ra, rb, rl, rr,
               x_sem, comb_send, comb_recv, ag_send, ag_recv, w_sem, rs_send, rs_recv):
    n, tok_dev, d_model, d_ff, n_exp, top_k, cap = dims
    chips = n // 2
    kw = d_model // KCHUNKS
    n_gate = 2 * KCHUNKS * n_exp
    wide = d_ff // 2
    n_items = n_gate + n_exp * (d_model // wide)
    n_chunks = d_model // COLS
    half_tok = n * tok_dev // 2
    half_slot = n * cap // 2

    me = lax.axis_index("ep")
    chip, core = me // 2, me % 2
    sibling = chip * 2 + (1 - core)
    c_right, c_left, c_opp = (chip + 1) % chips, (chip + chips - 1) % chips, (chip + 2) % chips
    right, left, opp = c_right * 2 + core, c_left * 2 + core, c_opp * 2 + core
    other = 1 - core

    def remote(src, dst, send, recv, dev):
        return pltpu.make_async_remote_copy(src_ref=src, dst_ref=dst, send_sem=send, recv_sem=recv,
                                            device_id={"ep": dev}, device_id_type=pl.DeviceIdType.MESH)

    def x_copy(kc):
        return pltpu.make_async_copy(x_hbm.at[:, pl.ds(kc * kw, kw)],
                                     xbuf.at[kc, pl.ds(pl.multiple_of(me * tok_dev, tok_dev), tok_dev), :], x_sem.at[kc])

    def ring_copy(src, slot, j):
        return pltpu.make_async_copy(src, ring.at[slot, pl.ds(j * kw, kw), :], w_sem.at[slot, j])

    def start_gate(kc, e, item):
        rows = pl.ds(pl.multiple_of(kc * kw, kw), kw)
        for which, w in enumerate((wg_hbm, wu_hbm)):
            for j in range(2):
                ring_copy(w.at[e, rows, pl.ds(j * wide, wide)], (item + which) % SLOTS, j).start()

    def start_down(c, e, item):
        cols = pl.ds(pl.multiple_of(c * wide, wide), wide)
        for j in range(2):
            ring_copy(wd_hbm.at[e, pl.ds(j * kw, kw), cols], item % SLOTS, j).start()

    def wait_slot(slot):
        for j in range(2):
            ring_copy(wd_hbm.at[0, pl.ds(j * kw, kw), pl.ds(0, wide)], slot, j).wait()

    for kc in range(KCHUNKS):
        x_copy(kc).start()
    for step in range(SLOTS // 2):
        start_gate(step // n_exp, step % n_exp, 2 * step)

    table[...] = jnp.zeros_like(table)
    mine = pl.ds(pl.multiple_of(core * tok_dev, tok_dev), tok_dev)
    table[mine, 0:top_k] = route_ref[...].astype(F32)
    table[mine, top_k:2 * top_k] = gate_ref[...]
    comb_in[...] = table[...].T[0:2 * top_k, :]

    barrier = pltpu.get_barrier_semaphore()
    for off in range(1, n):
        pl.semaphore_signal(barrier, inc=1, device_id={"ep": (me + off) % n}, device_id_type=pl.DeviceIdType.MESH)
    pl.semaphore_wait(barrier, n - 1)

    def block(kc, src):
        return xbuf.at[kc, pl.ds(pl.multiple_of(src * tok_dev, tok_dev), tok_dev), :]

    def ag_copy(kc, src, lane, dev):
        return remote(block(kc, src), block(kc, src), ag_send.at[kc, lane], ag_recv.at[kc, src], dev)

    def send_own(kc):
        x_copy(kc).wait()
        ag_copy(kc, me, 0, right).start()
        ag_copy(kc, me, 1, left).start()
        ag_copy(kc, me, 2, sibling).start()

    def relay_near(kc):
        ag_copy(kc, left, 3, sibling).wait_recv()
        ag_copy(kc, right, 4, sibling).wait_recv()
        if kc % 2 == 0:
            ag_copy(kc, left, 5, right).start()
        else:
            ag_copy(kc, right, 5, left).start()
        ag_copy(kc, left, 3, sibling).start()
        ag_copy(kc, right, 4, sibling).start()

    def relay_far(kc):
        ag_copy(kc, opp, 6, sibling).wait_recv()
        ag_copy(kc, opp, 6, sibling).start()

    def gathered(kc):
        for c in (chip, c_left, c_right, c_opp):
            ag_copy(kc, c * 2 + other, 2, sibling).wait_recv()

    send_own(0)
    comb_copies = []
    for off in range(1, n):
        copy = remote(comb_in, comb.at[me], comb_send.at[off - 1], comb_recv.at[me], (me + off) % n)
        copy.start()
        comb_copies.append(copy)
    comb[me] = comb_in[...]
    send_own(1)

    for off in range(1, n):
        src = (me + off) % n
        remote(comb_in, comb.at[src], comb_send.at[off - 1], comb_recv.at[src], src).wait_recv()

    lanes = 2 * tok_dev
    t_row = lax.broadcasted_iota(jnp.int32, (lanes, lanes), 0)
    t_col = lax.broadcasted_iota(jnp.int32, (lanes, lanes), 1)
    before = jnp.where((t_row < t_col) & (t_row // tok_dev == t_col // tok_dev), 1.0, 0.0).astype(BF16)
    e_id = (lax.broadcasted_iota(jnp.int32, (n_exp, lanes), 0) + me * n_exp).astype(F32)
    lane_base = ((lax.broadcasted_iota(jnp.int32, (n_exp, lanes), 1) // tok_dev) * cap).astype(F32)
    for c in range(chips):
        both = comb[2 * c] + comb[2 * c + 1]
        hits = jnp.zeros((n_exp, lanes), F32)
        gates = jnp.zeros((n_exp, lanes), F32)
        for k in range(top_k):
            same = jnp.broadcast_to(both[k:k + 1, :], (n_exp, lanes)) == e_id
            hits = hits + jnp.where(same, 1.0, 0.0)
            gates = gates + jnp.where(same, jnp.broadcast_to(both[top_k + k:top_k + k + 1, :], (n_exp, lanes)), 0.0)
        rank = jnp.dot(hits.astype(BF16), before, preferred_element_type=F32)
        code = jnp.where(hits > 0.0, rank + lane_base + float((c % 2) * 2 * cap), -1.0)
        codes[c, 0:n_exp, :] = code
        codes[c, n_exp:2 * n_exp, :] = gates

    def gather_tables(e, carry):
        slot_row = lax.broadcasted_iota(jnp.int32, (half_slot, lanes), 0).astype(F32)
        for c in range(chips):
            code = jnp.broadcast_to(codes[c, pl.ds(e, 1), :], (half_slot, lanes))
            pmat[e, c // 2, :, (c % 2) * lanes:(c % 2 + 1) * lanes] = jnp.where(code == slot_row, 1.0, 0.0).astype(BF16)
        return carry

    def scatter_tables(e, carry):
        slot_col = lax.broadcasted_iota(jnp.int32, (lanes, half_slot), 1).astype(F32)
        for c in range(chips):
            code = jnp.broadcast_to(codes[c, pl.ds(e, 1), :], (half_slot, lanes))
            smat[e, c * lanes:(c + 1) * lanes, :] = jnp.where(code.T == slot_col, 1.0, 0.0).astype(BF16)
            gate = jnp.broadcast_to(codes[c, pl.ds(n_exp + e, 1), :], (lanes, lanes))
            gmat[e, c * lanes:(c + 1) * lanes, :] = gate.T
        return carry

    relay_near(0)
    send_own(2)
    lax.fori_loop(0, n_exp, gather_tables, 0)
    relay_far(0)
    lax.fori_loop(0, n_exp, scatter_tables, 0)
    gathered(0)

    def expert_chunk(kc, e):
        step = kc * n_exp + e
        g_slot, u_slot = (2 * step) % SLOTS, (2 * step + 1) % SLOTS
        wait_slot(g_slot)
        wait_slot(u_slot)
        rows = [jnp.dot(pmat[e, h], xbuf[kc, h * half_tok:(h + 1) * half_tok, :], preferred_element_type=F32) for h in range(2)]
        xs = jnp.concatenate(rows, axis=0).astype(BF16)
        for c in range(d_ff // 256):
            cols = slice(c * 256, (c + 1) * 256)
            j, at = c * 256 // wide, c * 256 % wide
            g = jnp.dot(xs, ring[g_slot, j * kw:(j + 1) * kw, at:at + 256], preferred_element_type=F32)
            u = jnp.dot(xs, ring[u_slot, j * kw:(j + 1) * kw, at:at + 256], preferred_element_type=F32)
            if kc > 0:
                g = gacc[e, :, cols] + g
                u = uacc[e, :, cols] + u
            if kc < KCHUNKS - 1:
                gacc[e, :, cols] = g
                uacc[e, :, cols] = u
            else:
                hid[e, :, cols] = (jax.nn.silu(g) * u).astype(BF16)

        nxt = 2 * step + SLOTS

        @pl.when(nxt < n_gate)
        def _():
            start_gate(nxt // 2 // n_exp, nxt // 2 % n_exp, nxt)

        @pl.when((nxt >= n_gate) & (nxt < n_items))
        def _():
            for i in range(2):
                start_down((nxt + i - n_gate) // n_exp, (nxt + i - n_gate) % n_exp, nxt + i)

    for kc in range(KCHUNKS):
        def body(e, carry, kc=kc):
            expert_chunk(kc, e)
            nxt = kc + 1
            if nxt < KCHUNKS:
                @pl.when(e == 0)
                def _():
                    relay_near(nxt)
                    if nxt + 2 < KCHUNKS:
                        send_own(nxt + 2)

                @pl.when(e == n_exp // 2)
                def _():
                    relay_far(nxt)
            return carry

        lax.fori_loop(0, n_exp, body, 0)
        if kc + 1 < KCHUNKS:
            gathered(kc + 1)

    def to_sibling(c):
        return remote(acc.at[c, :, other], sib.at[c], rs_send.at[0, c], rs_recv.at[0, c], sibling)

    def far_right(c):
        return remote(acc.at[c, c_opp, core, :, pl.ds(0, COLS // 2)], ra.at[c], rs_send.at[1, c], rs_recv.at[1, c], right)

    def far_left(c):
        return remote(acc.at[c, c_opp, core, :, pl.ds(COLS // 2, COLS // 2)], rb.at[c], rs_send.at[2, c], rs_recv.at[2, c], left)

    def near_right(c):
        return remote(acc.at[c, c_right, core], rl.at[c], rs_send.at[3, c], rs_recv.at[3, c], right)

    def near_left(c):
        return remote(acc.at[c, c_left, core], rr.at[c], rs_send.at[4, c], rs_recv.at[4, c], left)

    def stage2(c):
        to_sibling(c).wait_recv()
        acc[c, :, core] = acc[c, :, core] + sib[c]
        far_right(c).start()
        far_left(c).start()

    def stage3(c):
        far_right(c).wait_recv()
        acc[c, c_right, core, :, :COLS // 2] = acc[c, c_right, core, :, :COLS // 2] + ra[c]
        near_right(c).start()
        far_left(c).wait_recv()
        acc[c, c_left, core, :, COLS // 2:] = acc[c, c_left, core, :, COLS // 2:] + rb[c]
        near_left(c).start()

    def stage4(c):
        near_right(c).wait_recv()
        near_left(c).wait_recv()
        y_ref[:, pl.ds(pl.multiple_of(c * COLS, COLS), COLS)] = (acc[c, chip, core] + rl[c] + rr[c]).astype(BF16)

    per = wide // COLS

    def down_item(c, e):
        return n_gate + (c // per) * n_exp + e

    def down(c):
        cols = pl.ds(pl.multiple_of((c % per) * COLS, COLS), COLS)
        for e in range(n_exp):
            slot = down_item(c, e) % SLOTS

            @pl.when(c % per == 0)
            def _():
                wait_slot(slot)
        for e in range(n_exp):
            slot = down_item(c, e) % SLOTS
            outs[e] = jnp.dot(hid[e], ring[slot, :, cols], preferred_element_type=F32).astype(BF16)

    def put_back(c):
        for ch in range(chips):
            total = None
            for e in range(n_exp):
                put = jnp.dot(smat[e, ch * lanes:(ch + 1) * lanes, :], outs[e, (ch // 2) * half_slot:(ch // 2 + 1) * half_slot, :],
                              preferred_element_type=F32)
                gate = gmat[e, ch * lanes:(ch + 1) * lanes, :]
                put = put * jnp.concatenate([gate] * (COLS // lanes), axis=1)
                total = put if total is None else total + put
            acc[c, ch] = total.reshape(2, tok_dev, COLS)

        @pl.when(c % per == per - 1)
        def _():
            for e in range(n_exp):
                nxt = down_item(c, e) + SLOTS

                @pl.when(nxt < n_items)
                def _():
                    start_down((nxt - n_gate) // n_exp, (nxt - n_gate) % n_exp, nxt)

    def chunk_body(c, carry):
        down(c)

        @pl.when(c >= 1)
        def _():
            stage2(c - 1)
        put_back(c)
        to_sibling(c).start()

        @pl.when(c >= 2)
        def _():
            stage3(c - 2)

        @pl.when(c >= 3)
        def _():
            stage4(c - 3)
        return carry

    lax.fori_loop(0, n_chunks, chunk_body, 0)
    last = n_chunks - 1
    stage2(last)
    stage3(last - 1)
    stage4(last - 2)
    stage3(last)
    stage4(last - 1)
    stage4(last)

    for copy in comb_copies:
        copy.wait_send()
    for kc in range(KCHUNKS):
        for lane, (src, dev) in enumerate(((me, right), (me, left), (me, sibling), (left, sibling), (right, sibling),
                                           (left, right) if kc % 2 == 0 else (right, left), (opp, sibling))):
            ag_copy(kc, src, lane, dev).wait_send()

    def drain(c, carry):
        for make in (to_sibling, far_right, far_left, near_right, near_left):
            make(c).wait_send()
        return carry

    lax.fori_loop(0, n_chunks, drain, 0)


def solution(mesh):
    n = mesh.shape["ep"]
    row_spec = P(("dp", "ep"))
    expert_spec = P("ep")

    def local_step(tok, route, gate, wg, wu, wd):
        tok_dev, d_model = tok.shape
        n_exp, _, d_ff = wg.shape
        top_k = route.shape[1]
        cap = tok_dev // 2
        chips = n // 2
        lanes = 2 * tok_dev
        kw = d_model // KCHUNKS
        n_chunks = d_model // COLS
        dims = (n, tok_dev, d_model, d_ff, n_exp, top_k, cap)

        hbm = pl.BlockSpec(memory_space=pl.ANY)
        vmem = pl.BlockSpec(memory_space=pltpu.VMEM)
        return pl.pallas_call(
            functools.partial(moe_kernel, dims),
            out_shape=jax.ShapeDtypeStruct((tok_dev, d_model), BF16),
            in_specs=[hbm, vmem, vmem, hbm, hbm, hbm],
            out_specs=vmem,
            scratch_shapes=[
                pltpu.VMEM((KCHUNKS, n * tok_dev, kw), BF16),
                pltpu.VMEM((lanes, lanes), F32),
                pltpu.VMEM((2 * top_k, lanes), F32),
                pltpu.VMEM((n, 2 * top_k, lanes), F32),
                pltpu.VMEM((chips, 2 * n_exp, lanes), F32),
                pltpu.VMEM((n_exp, 2, n * cap // 2, n * tok_dev // 2), BF16),
                pltpu.VMEM((n_exp, n * tok_dev, n * cap // 2), BF16),
                pltpu.VMEM((n_exp, n * tok_dev, lanes), F32),
                pltpu.VMEM((n_exp, n * cap, d_ff), F32),
                pltpu.VMEM((n_exp, n * cap, d_ff), F32),
                pltpu.VMEM((n_exp, n * cap, d_ff), BF16),
                pltpu.VMEM((SLOTS, 2 * kw, d_ff // 2), BF16),
                pltpu.VMEM((n_exp, n * cap, COLS), BF16),
                pltpu.VMEM((n_chunks, chips, 2, tok_dev, COLS), F32),
                pltpu.VMEM((n_chunks, chips, tok_dev, COLS), F32),
                pltpu.VMEM((n_chunks, tok_dev, COLS // 2), F32),
                pltpu.VMEM((n_chunks, tok_dev, COLS // 2), F32),
                pltpu.VMEM((n_chunks, tok_dev, COLS), F32),
                pltpu.VMEM((n_chunks, tok_dev, COLS), F32),
                pltpu.SemaphoreType.DMA((KCHUNKS,)),
                pltpu.SemaphoreType.DMA((n - 1,)),
                pltpu.SemaphoreType.DMA((n,)),
                pltpu.SemaphoreType.DMA((KCHUNKS, 7)),
                pltpu.SemaphoreType.DMA((KCHUNKS, n)),
                pltpu.SemaphoreType.DMA((SLOTS, 2)),
                pltpu.SemaphoreType.DMA((5, n_chunks)),
                pltpu.SemaphoreType.DMA((5, n_chunks)),
            ],
            compiler_params=pltpu.CompilerParams(collective_id=0, has_side_effects=True, vmem_limit_bytes=67_043_328),
        )(tok, route, gate, wg, wu, wd)

    return jax.shard_map(local_step, mesh=mesh, in_specs=(row_spec, row_spec, row_spec, expert_spec, expert_spec, expert_spec), out_specs=row_spec, check_vma=False)
```

```python
import functools

import jax
import jax.numpy as jnp
from jax import lax
from jax.experimental import pallas as pl
from jax.experimental.pallas import tpu as pltpu
from jax.sharding import PartitionSpec as P

F32 = jnp.float32
BF16 = jnp.bfloat16
KCHUNKS = 4
COLS = 256
SLOTS = 22
FILL = (4, 8, SLOTS // 2)


def moe_kernel(dims, x_hbm, route_ref, gate_ref, wg_hbm, wu_hbm, wd_hbm, y_ref,
               xbuf, comb_in, comb, codes, pmat, smat, gmat, xs, gacc, uacc, hid, ring, outs, acc, sib, ra, rb, rl, rr,
               x_sem, comb_send, comb_recv, ag_send, ag_recv, w_sem, rs_send, rs_recv):
    n, tok_dev, d_model, d_ff, n_exp, top_k, cap = dims
    chips = n // 2
    lanes = 2 * tok_dev
    kw = d_model // KCHUNKS
    n_steps = KCHUNKS * n_exp
    single = 2 * n_exp
    n_gate = 2 * n_steps
    wide = d_ff // 2
    n_items = n_gate + n_exp * (d_model // wide)
    n_chunks = d_model // COLS
    half_tok = n * tok_dev // 2
    half_slot = n * cap // 2

    me = lax.axis_index("ep")
    chip, core = me // 2, me % 2
    other = 1 - core
    sibling = chip * 2 + other
    c_right, c_left, c_opp = (chip + 1) % chips, (chip + chips - 1) % chips, (chip + 2) % chips
    right, left, opp = c_right * 2 + core, c_left * 2 + core, c_opp * 2 + core

    def remote(src, dst, send, recv, dev):
        return pltpu.make_async_remote_copy(src_ref=src, dst_ref=dst, send_sem=send, recv_sem=recv,
                                            device_id={"ep": dev}, device_id_type=pl.DeviceIdType.MESH)

    def x_copy(kc):
        return pltpu.make_async_copy(x_hbm.at[:, pl.ds(kc * kw, kw)],
                                     xbuf.at[kc, pl.ds(pl.multiple_of(me * tok_dev, tok_dev), tok_dev), :], x_sem.at[kc])

    def gate_copy(w, kc, e, slot):
        return pltpu.make_async_copy(w.at[e, pl.ds(pl.multiple_of(kc * kw, kw), kw), :], ring.at[slot], w_sem.at[slot])

    def wait_slot(slot):
        gate_copy(wg_hbm, 0, 0, slot).wait()

    def start_pair(kc, e, item):
        gate_copy(wg_hbm, kc, e, item % SLOTS).start()
        gate_copy(wu_hbm, kc, e, (item + 1) % SLOTS).start()

    def start_down(item):
        c, e, slot = (item - n_gate) // n_exp, (item - n_gate) % n_exp, item % SLOTS
        cols = pl.ds(pl.multiple_of(c * wide, wide), wide)
        for j in range(2):
            pltpu.make_async_copy(wd_hbm.at[e, pl.ds(j * kw, kw), cols], ring.at[slot, :, pl.ds(j * wide, wide)], w_sem.at[slot]).start()

    def start_step(step):
        @pl.when(step < single)
        def _():
            start_pair(step // n_exp, step % n_exp, 2 * step)

        @pl.when((step >= single) & (step < n_steps))
        def _():
            start_pair(2 + step % 2, (step - single) // 2, 2 * step)

        @pl.when((step >= n_steps) & (2 * step < n_items))
        def _():
            start_down(2 * step)
            start_down(2 * step + 1)

    def fill(part):
        for step in range(FILL[part - 1] if part else 0, FILL[part]):
            start_pair(step // n_exp, step % n_exp, 2 * step)

    for kc in range(KCHUNKS):
        x_copy(kc).start()
    fill(0)

    mine = lax.broadcasted_iota(jnp.int32, (top_k, lanes), 1) // tok_dev == core
    for i, part in enumerate((route_ref[...].astype(F32), gate_ref[...])):
        comb_in[i * top_k:(i + 1) * top_k, :] = jnp.where(mine, jnp.concatenate([part, part], axis=1), 0.0)

    barrier = pltpu.get_barrier_semaphore()
    for off in range(1, n):
        pl.semaphore_signal(barrier, inc=1, device_id={"ep": (me + off) % n}, device_id_type=pl.DeviceIdType.MESH)
    pl.semaphore_wait(barrier, n - 1)

    def blocks(kc, first, count=1):
        return xbuf.at[kc, pl.ds(pl.multiple_of(first * tok_dev, tok_dev), count * tok_dev), :]

    def ag_copy(kc, src, dev, over_chip):
        return remote(blocks(kc, src), blocks(kc, src), ag_send, ag_recv.at[kc, over_chip], dev)

    def send_own(kc):
        for dev in (right, left, opp):
            ag_copy(kc, me, dev, 0).start()
        ag_copy(kc, me, sibling, 1).start()

    def forward(kc):
        remote(blocks(kc, 0, chips - 1), blocks(kc, 0, chips - 1), ag_send, ag_recv.at[kc, 0], sibling).wait_recv()
        for src in (left, right, opp):
            ag_copy(kc, src, sibling, 1).start()

    def gathered(kc):
        remote(blocks(kc, 0, chips), blocks(kc, 0, chips), ag_send, ag_recv.at[kc, 1], sibling).wait_recv()

    x_copy(0).wait()
    send_own(0)
    for off in range(1, n):
        remote(comb_in, comb.at[me], comb_send, comb_recv, (me + off) % n).start()
    comb[me] = comb_in[...]
    for kc in range(1, KCHUNKS):
        x_copy(kc).wait()
        send_own(kc)
    fill(1)
    comb_all = remote(comb.at[pl.ds(0, n - 1)], comb.at[pl.ds(0, n - 1)], comb_send, comb_recv, sibling)
    comb_all.wait_recv()

    t_row = lax.broadcasted_iota(jnp.int32, (lanes, lanes), 0)
    t_col = lax.broadcasted_iota(jnp.int32, (lanes, lanes), 1)
    before = jnp.where((t_row < t_col) & (t_row // tok_dev == t_col // tok_dev), 1.0, 0.0).astype(BF16)
    e_id = (lax.broadcasted_iota(jnp.int32, (n_exp, lanes), 0) + me * n_exp).astype(F32)
    lane_base = ((lax.broadcasted_iota(jnp.int32, (n_exp, lanes), 1) // tok_dev) * cap).astype(F32)
    for c in range(chips):
        both = comb[2 * c] + comb[2 * c + 1]
        hits = jnp.zeros((n_exp, lanes), F32)
        gates = jnp.zeros((n_exp, lanes), F32)
        for k in range(top_k):
            same = jnp.broadcast_to(both[k:k + 1, :], (n_exp, lanes)) == e_id
            hits = hits + jnp.where(same, 1.0, 0.0)
            gates = gates + jnp.where(same, jnp.broadcast_to(both[top_k + k:top_k + k + 1, :], (n_exp, lanes)), 0.0)
        rank = jnp.dot(hits.astype(BF16), before, preferred_element_type=F32)
        code = jnp.where(hits > 0.0, rank + lane_base + float((c % 2) * 2 * cap), -1.0)
        codes[c, 0:n_exp, :] = code
        codes[c, n_exp:2 * n_exp, :] = gates

    def gather_tables(e, carry):
        slot_row = lax.broadcasted_iota(jnp.int32, (half_slot, lanes), 0).astype(F32)
        for c in range(chips):
            code = jnp.broadcast_to(codes[c, pl.ds(e, 1), :], (half_slot, lanes))
            pmat[c // 2, e, :, (c % 2) * lanes:(c % 2 + 1) * lanes] = jnp.where(code == slot_row, 1.0, 0.0).astype(BF16)
        return carry

    def scatter_tables(e):
        slot_col = lax.broadcasted_iota(jnp.int32, (lanes, half_slot), 1).astype(F32)
        for c in range(chips):
            code = jnp.broadcast_to(codes[c, pl.ds(e, 1), :], (half_slot, lanes))
            smat[e, c * lanes:(c + 1) * lanes, :] = jnp.where(code.T == slot_col, 1.0, 0.0).astype(BF16)
            gate = jnp.broadcast_to(codes[c, pl.ds(n_exp + e, 1), :], (lanes, lanes))
            gmat[e, c * lanes:(c + 1) * lanes, :] = gate.T

    lax.fori_loop(0, n_exp, gather_tables, 0)
    forward(0)
    fill(2)

    def gather(kc, g):
        gathered(kc)
        for h in range(2):
            picks = pmat[h].reshape(n_exp * half_slot, half_tok)
            for at in range(0, kw, 256):
                rows = jnp.dot(picks, xbuf[kc, h * half_tok:(h + 1) * half_tok, at:at + 256], preferred_element_type=F32)
                xs[g, :, h, :, at:at + 256] = rows.astype(BF16).reshape(n_exp, half_slot, 256)

    def expert_pass(e, slots, groups, first, last):
        for at in range(0, d_ff, 256):
            cols = slice(at, at + 256)
            g = u = None
            for i in range(groups):
                rows = xs[i, e].reshape(2 * half_slot, kw)
                dg = jnp.dot(rows, ring[slots[2 * i], :, cols], preferred_element_type=F32)
                du = jnp.dot(rows, ring[slots[2 * i + 1], :, cols], preferred_element_type=F32)
                g, u = (dg, du) if g is None else (g + dg, u + du)
            if not first:
                g = gacc[e, :, cols] + g
                u = uacc[e, :, cols] + u
            if last:
                hid[e, :, cols] = (jax.nn.silu(g) * u).astype(BF16)
            else:
                gacc[e, :, cols] = g
                uacc[e, :, cols] = u

    def take(step, count):
        slots = [(2 * step + i) % SLOTS for i in range(2 * count)]
        for slot in slots:
            wait_slot(slot)
        return slots

    def refill(step, count):
        for i in range(count):
            start_step(step + i + SLOTS // 2)

    for kc in range(2):
        def pair_body(i, carry, kc=kc):
            step = kc * n_exp + 2 * i
            slots = take(step, 2)
            for j in range(2):
                if kc == 0:
                    scatter_tables(2 * i + j)
                expert_pass(2 * i + j, slots[2 * j:2 * j + 2], 1, kc == 0, False)
            refill(step, 2)
            if kc == 0:
                @pl.when(i == n_exp // 2 - 2)
                def _():
                    forward(1)
            else:
                @pl.when(i == 0)
                def _():
                    forward(2)

                @pl.when(i == n_exp // 2 - 2)
                def _():
                    forward(3)
            return carry

        gather(kc, 0)
        lax.fori_loop(0, n_exp // 2, pair_body, 0)

    def last_body(e, carry):
        step = single + 2 * e
        slots = take(step, 2)
        expert_pass(e, slots, 2, False, True)
        refill(step, 2)
        return carry

    gather(2, 0)
    gather(3, 1)
    lax.fori_loop(0, n_exp, last_body, 0)

    half = COLS // 2

    def to_sibling(c):
        return remote(acc.at[c, :, other], sib.at[c], rs_send.at[0], rs_recv.at[0, c], sibling)

    def far_right(c):
        return remote(acc.at[c, c_opp, core, :, pl.ds(0, half)], ra.at[c], rs_send.at[1], rs_recv.at[1, c], right)

    def far_left(c):
        return remote(acc.at[c, c_opp, core, :, pl.ds(half, half)], rb.at[c], rs_send.at[2], rs_recv.at[2, c], left)

    def near_right(c, j):
        cols = pl.ds(j * half, half)
        return remote(acc.at[c, c_right, core, :, cols], rl.at[c, :, cols], rs_send.at[3], rs_recv.at[3, c], right)

    def near_left(c, j):
        cols = pl.ds(j * half, half)
        return remote(acc.at[c, c_left, core, :, cols], rr.at[c, :, cols], rs_send.at[4], rs_recv.at[4, c], left)

    def stage2(c):
        to_sibling(c).wait_recv()
        acc[c, :, core] = acc[c, :, core] + sib[c]
        far_right(c).start()
        far_left(c).start()
        near_right(c, 1).start()
        near_left(c, 0).start()

    def stage3(c):
        far_right(c).wait_recv()
        acc[c, c_right, core, :, :half] = acc[c, c_right, core, :, :half] + ra[c]
        near_right(c, 0).start()
        far_left(c).wait_recv()
        acc[c, c_left, core, :, half:] = acc[c, c_left, core, :, half:] + rb[c]
        near_left(c, 1).start()

    def stage4(c):
        remote(rl.at[c], rl.at[c], rs_send.at[3], rs_recv.at[3, c], right).wait_recv()
        remote(rr.at[c], rr.at[c], rs_send.at[4], rs_recv.at[4, c], left).wait_recv()
        y_ref[:, pl.ds(pl.multiple_of(c * COLS, COLS), COLS)] = (acc[c, chip, core] + rl[c] + rr[c]).astype(BF16)

    per = wide // COLS

    def down_item(c, e):
        return n_gate + (c // per) * n_exp + e

    def down(c):
        @pl.when(c % per == 0)
        def _():
            for e in range(n_exp):
                wait_slot(down_item(c, e) % SLOTS)
        for e in range(n_exp):
            slot = down_item(c, e) % SLOTS
            parts = [jnp.dot(hid[e, :, j * kw:(j + 1) * kw],
                             ring[slot, :, pl.ds(pl.multiple_of(j * wide + (c % per) * COLS, COLS), COLS)], preferred_element_type=F32)
                     for j in range(2)]
            outs[e] = (parts[0] + parts[1]).astype(BF16)

    def put_back(c):
        for ch in range(chips):
            total = None
            for e in range(n_exp):
                put = jnp.dot(smat[e, ch * lanes:(ch + 1) * lanes, :], outs[e, (ch // 2) * half_slot:(ch // 2 + 1) * half_slot, :],
                              preferred_element_type=F32)
                gate = gmat[e, ch * lanes:(ch + 1) * lanes, :]
                put = put * jnp.concatenate([gate] * (COLS // lanes), axis=1)
                total = put if total is None else total + put
            acc[c, ch] = total.reshape(2, tok_dev, COLS)

        @pl.when(c % per == per - 1)
        def _():
            for e in range(n_exp):
                nxt = down_item(c, e) + SLOTS

                @pl.when(nxt < n_items)
                def _():
                    start_down(nxt)

    def chunk_body(c, carry):
        down(c)

        @pl.when(c >= 1)
        def _():
            stage2(c - 1)
        put_back(c)
        to_sibling(c).start()

        @pl.when(c >= 2)
        def _():
            stage3(c - 2)

        @pl.when(c >= 4)
        def _():
            stage4(c - 4)
        return carry

    lax.fori_loop(0, n_chunks, chunk_body, 0)
    last = n_chunks - 1
    stage2(last)
    stage3(last - 1)
    stage4(last - 3)
    stage3(last)
    for c in range(last - 2, n_chunks):
        stage4(c)

    comb_all.wait_send()
    everything = xbuf.at[:, pl.ds(0, (2 * chips - 1) * tok_dev), :]
    remote(everything, everything, ag_send, ag_recv.at[0, 0], sibling).wait_send()
    for i, ref in enumerate((sib, ra, rb, rl, rr)):
        remote(ref, ref, rs_send.at[i], rs_recv.at[i, 0], sibling).wait_send()


def solution(mesh):
    n = mesh.shape["ep"]
    row_spec = P(("dp", "ep"))
    expert_spec = P("ep")

    def local_step(tok, route, gate, wg, wu, wd):
        tok_dev, d_model = tok.shape
        n_exp, _, d_ff = wg.shape
        top_k = route.shape[1]
        cap = tok_dev // 2
        chips = n // 2
        lanes = 2 * tok_dev
        kw = d_model // KCHUNKS
        n_chunks = d_model // COLS
        dims = (n, tok_dev, d_model, d_ff, n_exp, top_k, cap)

        hbm = pl.BlockSpec(memory_space=pl.ANY)
        vmem = pl.BlockSpec(memory_space=pltpu.VMEM)
        return pl.pallas_call(
            functools.partial(moe_kernel, dims),
            out_shape=jax.ShapeDtypeStruct((tok_dev, d_model), BF16),
            in_specs=[hbm, vmem, vmem, hbm, hbm, hbm],
            out_specs=vmem,
            scratch_shapes=[
                pltpu.VMEM((KCHUNKS, n * tok_dev, kw), BF16),
                pltpu.VMEM((2 * top_k, lanes), F32),
                pltpu.VMEM((n, 2 * top_k, lanes), F32),
                pltpu.VMEM((chips, 2 * n_exp, lanes), F32),
                pltpu.VMEM((2, n_exp, n * cap // 2, n * tok_dev // 2), BF16),
                pltpu.VMEM((n_exp, n * tok_dev, n * cap // 2), BF16),
                pltpu.VMEM((n_exp, n * tok_dev, lanes), F32),
                pltpu.VMEM((2, n_exp, 2, n * cap // 2, kw), BF16),
                pltpu.VMEM((n_exp, n * cap, d_ff), F32),
                pltpu.VMEM((n_exp, n * cap, d_ff), F32),
                pltpu.VMEM((n_exp, n * cap, d_ff), BF16),
                pltpu.VMEM((SLOTS, kw, d_ff), BF16),
                pltpu.VMEM((n_exp, n * cap, COLS), BF16),
                pltpu.VMEM((n_chunks, chips, 2, tok_dev, COLS), F32),
                pltpu.VMEM((n_chunks, chips, tok_dev, COLS), F32),
                pltpu.VMEM((n_chunks, tok_dev, COLS // 2), F32),
                pltpu.VMEM((n_chunks, tok_dev, COLS // 2), F32),
                pltpu.VMEM((n_chunks, tok_dev, COLS), F32),
                pltpu.VMEM((n_chunks, tok_dev, COLS), F32),
                pltpu.SemaphoreType.DMA((KCHUNKS,)),
                pltpu.SemaphoreType.DMA,
                pltpu.SemaphoreType.DMA,
                pltpu.SemaphoreType.DMA,
                pltpu.SemaphoreType.DMA((KCHUNKS, 2)),
                pltpu.SemaphoreType.DMA((SLOTS,)),
                pltpu.SemaphoreType.DMA((5,)),
                pltpu.SemaphoreType.DMA((5, n_chunks)),
            ],
            compiler_params=pltpu.CompilerParams(collective_id=0, has_side_effects=True, vmem_limit_bytes=67_043_328),
        )(tok, route.T, gate.T, wg, wu, wd)

    return jax.shard_map(local_step, mesh=mesh, in_specs=(row_spec, row_spec, row_spec, expert_spec, expert_spec, expert_spec), out_specs=row_spec, check_vma=False)
```

```python
import functools

import jax
import jax.numpy as jnp
from jax import lax
from jax.experimental import pallas as pl
from jax.experimental.pallas import tpu as pltpu
from jax.sharding import PartitionSpec as P

F32 = jnp.float32
BF16 = jnp.bfloat16
KCHUNKS = 4
COLS = 256
SLOTS = 22
FILL = (4, 8, SLOTS // 2)


def moe_kernel(dims, x_hbm, route_ref, gate_ref, wg_hbm, wu_hbm, wd_hbm, y_ref,
               xbuf, comb_in, comb, codes, pmat, smat, gmat, xs, gacc, uacc, hid, ring, outs, acc, sib, ra, rb, rl, rr,
               x_sem, comb_send, comb_recv, ag_send, ag_recv, w_sem, rs_send, rs_recv):
    n, tok_dev, d_model, d_ff, n_exp, top_k, cap = dims
    chips = n // 2
    lanes = 2 * tok_dev
    kw = d_model // KCHUNKS
    n_steps = KCHUNKS * n_exp
    single = 2 * n_exp
    n_gate = 2 * n_steps
    wide = d_ff // 2
    n_items = n_gate + n_exp * (d_model // wide)
    n_chunks = d_model // COLS
    half_tok = n * tok_dev // 2
    half_slot = n * cap // 2

    me = lax.axis_index("ep")
    chip, core = me // 2, me % 2
    other = 1 - core
    sibling = chip * 2 + other
    c_right, c_left, c_opp = (chip + 1) % chips, (chip + chips - 1) % chips, (chip + 2) % chips
    right, left, opp = c_right * 2 + core, c_left * 2 + core, c_opp * 2 + core

    def remote(src, dst, send, recv, dev):
        return pltpu.make_async_remote_copy(src_ref=src, dst_ref=dst, send_sem=send, recv_sem=recv,
                                            device_id={"ep": dev}, device_id_type=pl.DeviceIdType.MESH)

    def x_copy(kc):
        return pltpu.make_async_copy(x_hbm.at[:, pl.ds(kc * kw, kw)],
                                     xbuf.at[kc, pl.ds(pl.multiple_of(me * tok_dev, tok_dev), tok_dev), :], x_sem.at[kc])

    def gate_copy(w, kc, e, slot):
        return pltpu.make_async_copy(w.at[e, pl.ds(pl.multiple_of(kc * kw, kw), kw), :], ring.at[slot], w_sem.at[slot])

    def wait_slot(slot):
        gate_copy(wg_hbm, 0, 0, slot).wait()

    def start_pair(kc, e, item):
        gate_copy(wg_hbm, kc, e, item % SLOTS).start()
        gate_copy(wu_hbm, kc, e, (item + 1) % SLOTS).start()

    def start_down(item):
        c, e, slot = (item - n_gate) // n_exp, (item - n_gate) % n_exp, item % SLOTS
        cols = pl.ds(pl.multiple_of(c * wide, wide), wide)
        for j in range(2):
            pltpu.make_async_copy(wd_hbm.at[e, pl.ds(j * kw, kw), cols], ring.at[slot, :, pl.ds(j * wide, wide)], w_sem.at[slot]).start()

    def start_step(step):
        @pl.when(step < single)
        def _():
            start_pair(step // n_exp, step % n_exp, 2 * step)

        @pl.when((step >= single) & (step < n_steps))
        def _():
            start_pair(2 + step % 2, (step - single) // 2, 2 * step)

        @pl.when((step >= n_steps) & (2 * step < n_items))
        def _():
            start_down(2 * step)
            start_down(2 * step + 1)

    def fill(part):
        for step in range(FILL[part - 1] if part else 0, FILL[part]):
            start_pair(step // n_exp, step % n_exp, 2 * step)

    for kc in range(KCHUNKS):
        x_copy(kc).start()
    fill(0)

    mine = lax.broadcasted_iota(jnp.int32, (top_k, lanes), 1) // tok_dev == core
    for i, part in enumerate((route_ref[...].astype(F32), gate_ref[...])):
        comb_in[i * top_k:(i + 1) * top_k, :] = jnp.where(mine, jnp.concatenate([part, part], axis=1), 0.0)

    barrier = pltpu.get_barrier_semaphore()
    for off in range(1, n):
        pl.semaphore_signal(barrier, inc=1, device_id={"ep": (me + off) % n}, device_id_type=pl.DeviceIdType.MESH)
    pl.semaphore_wait(barrier, n - 1)

    def blocks(kc, first, count=1):
        return xbuf.at[kc, pl.ds(pl.multiple_of(first * tok_dev, tok_dev), count * tok_dev), :]

    def ag_copy(kc, src, dev, over_chip):
        return remote(blocks(kc, src), blocks(kc, src), ag_send, ag_recv.at[kc, over_chip], dev)

    def send_own(kc):
        for dev in (right, left, opp):
            ag_copy(kc, me, dev, 0).start()
        ag_copy(kc, me, sibling, 1).start()

    def forward(kc):
        remote(blocks(kc, 0, chips - 1), blocks(kc, 0, chips - 1), ag_send, ag_recv.at[kc, 0], sibling).wait_recv()
        for src in (left, right, opp):
            ag_copy(kc, src, sibling, 1).start()

    def gathered(kc):
        remote(blocks(kc, 0, chips), blocks(kc, 0, chips), ag_send, ag_recv.at[kc, 1], sibling).wait_recv()

    def table_copy(i, dev):
        rows = pl.ds(i * top_k, top_k)
        return remote(comb_in.at[rows, :], comb.at[me, rows, :], comb_send.at[i], comb_recv.at[i], dev)

    def table_all(i):
        part = comb.at[pl.ds(0, n - 1), pl.ds(i * top_k, top_k), :]
        return remote(part, part, comb_send.at[i], comb_recv.at[i], sibling)

    for off in range(1, n):
        table_copy(0, (me + off) % n).start()
    comb[me] = comb_in[...]
    x_copy(0).wait()
    send_own(0)
    for off in range(1, n):
        table_copy(1, (me + off) % n).start()
    for kc in range(1, KCHUNKS):
        x_copy(kc).wait()
        send_own(kc)
    fill(1)
    table_all(0).wait_recv()

    t_row = lax.broadcasted_iota(jnp.int32, (lanes, lanes), 0)
    t_col = lax.broadcasted_iota(jnp.int32, (lanes, lanes), 1)
    before = jnp.where((t_row < t_col) & (t_row // tok_dev == t_col // tok_dev), 1.0, 0.0).astype(BF16)
    e_id = (lax.broadcasted_iota(jnp.int32, (n_exp, lanes), 0) + me * n_exp).astype(F32)
    lane_base = ((lax.broadcasted_iota(jnp.int32, (n_exp, lanes), 1) // tok_dev) * cap).astype(F32)
    for c in range(chips):
        route = comb[2 * c, 0:top_k] + comb[2 * c + 1, 0:top_k]
        hits = jnp.zeros((n_exp, lanes), F32)
        for k in range(top_k):
            hits = hits + jnp.where(jnp.broadcast_to(route[k:k + 1, :], (n_exp, lanes)) == e_id, 1.0, 0.0)
        rank = jnp.dot(hits.astype(BF16), before, preferred_element_type=F32)
        codes[c, 0:n_exp, :] = jnp.where(hits > 0.0, rank + lane_base + float((c % 2) * 2 * cap), -1.0)

    def gate_codes():
        table_all(1).wait_recv()
        for c in range(chips):
            both = comb[2 * c] + comb[2 * c + 1]
            gates = jnp.zeros((n_exp, lanes), F32)
            for k in range(top_k):
                same = jnp.broadcast_to(both[k:k + 1, :], (n_exp, lanes)) == e_id
                gates = gates + jnp.where(same, jnp.broadcast_to(both[top_k + k:top_k + k + 1, :], (n_exp, lanes)), 0.0)
            codes[c, n_exp:2 * n_exp, :] = gates

    def gather_tables(e, carry):
        slot_row = lax.broadcasted_iota(jnp.int32, (half_slot, lanes), 0).astype(F32)
        for c in range(chips):
            code = jnp.broadcast_to(codes[c, pl.ds(e, 1), :], (half_slot, lanes))
            pmat[c // 2, e, :, (c % 2) * lanes:(c % 2 + 1) * lanes] = jnp.where(code == slot_row, 1.0, 0.0).astype(BF16)
        return carry

    def scatter_tables(e):
        slot_col = lax.broadcasted_iota(jnp.int32, (lanes, half_slot), 1).astype(F32)
        for c in range(chips):
            code = jnp.broadcast_to(codes[c, pl.ds(e, 1), :], (half_slot, lanes))
            smat[e, c * lanes:(c + 1) * lanes, :] = jnp.where(code.T == slot_col, 1.0, 0.0).astype(BF16)
            gate = jnp.broadcast_to(codes[c, pl.ds(n_exp + e, 1), :], (lanes, lanes))
            gmat[e, c * lanes:(c + 1) * lanes, :] = gate.T

    lax.fori_loop(0, n_exp, gather_tables, 0)
    forward(0)
    fill(2)
    gate_codes()

    def gather(kc, g):
        gathered(kc)
        for h in range(2):
            picks = pmat[h].reshape(n_exp * half_slot, half_tok)
            for at in range(0, kw, 256):
                rows = jnp.dot(picks, xbuf[kc, h * half_tok:(h + 1) * half_tok, at:at + 256], preferred_element_type=F32)
                xs[g, :, h, :, at:at + 256] = rows.astype(BF16).reshape(n_exp, half_slot, 256)

    def expert_pass(e, slots, groups, first, last):
        for at in range(0, d_ff, 256):
            cols = slice(at, at + 256)
            g = u = None
            for i in range(groups):
                rows = xs[i, e].reshape(2 * half_slot, kw)
                dg = jnp.dot(rows, ring[slots[2 * i], :, cols], preferred_element_type=F32)
                du = jnp.dot(rows, ring[slots[2 * i + 1], :, cols], preferred_element_type=F32)
                g, u = (dg, du) if g is None else (g + dg, u + du)
            if not first:
                g = gacc[e, :, cols] + g
                u = uacc[e, :, cols] + u
            if last:
                hid[e, :, cols] = (jax.nn.silu(g) * u).astype(BF16)
            else:
                gacc[e, :, cols] = g
                uacc[e, :, cols] = u

    def take(step, count):
        slots = [(2 * step + i) % SLOTS for i in range(2 * count)]
        for slot in slots:
            wait_slot(slot)
        return slots

    def refill(step, count):
        for i in range(count):
            start_step(step + i + SLOTS // 2)

    for kc in range(2):
        def pair_body(i, carry, kc=kc):
            step = kc * n_exp + 2 * i
            slots = take(step, 2)
            for j in range(2):
                if kc == 0:
                    scatter_tables(2 * i + j)
                expert_pass(2 * i + j, slots[2 * j:2 * j + 2], 1, kc == 0, False)
            refill(step, 2)
            if kc == 0:
                @pl.when(i == n_exp // 2 - 2)
                def _():
                    forward(1)
            else:
                @pl.when(i == 0)
                def _():
                    forward(2)

                @pl.when(i == n_exp // 2 - 2)
                def _():
                    forward(3)
            return carry

        gather(kc, 0)
        lax.fori_loop(0, n_exp // 2, pair_body, 0)

    def last_body(i, carry):
        step = single + 4 * i
        slots = take(step, 4)
        for j in range(2):
            expert_pass(2 * i + j, slots[4 * j:4 * j + 4], 2, False, True)
        refill(step, 4)
        return carry

    gather(2, 0)
    gather(3, 1)
    lax.fori_loop(0, n_exp // 2, last_body, 0)

    half = COLS // 2

    def to_sibling(c):
        return remote(acc.at[c, :, other], sib.at[c], rs_send.at[0], rs_recv.at[0, c], sibling)

    def far_right(c):
        return remote(acc.at[c, c_opp, core, 0], ra.at[c], rs_send.at[1], rs_recv.at[1, c], right)

    def far_left(c):
        return remote(acc.at[c, c_opp, core, 1], rb.at[c], rs_send.at[2], rs_recv.at[2, c], left)

    def near_right(c, j):
        return remote(acc.at[c, c_right, core, j], rl.at[c, j], rs_send.at[3], rs_recv.at[3, c], right)

    def near_left(c, j):
        return remote(acc.at[c, c_left, core, j], rr.at[c, j], rs_send.at[4], rs_recv.at[4, c], left)

    def stage2(c):
        to_sibling(c).wait_recv()
        acc[c, :, core] = acc[c, :, core] + sib[c]
        far_right(c).start()
        far_left(c).start()
        near_right(c, 1).start()
        near_left(c, 0).start()

    def stage3(c):
        far_right(c).wait_recv()
        acc[c, c_right, core, 0] = acc[c, c_right, core, 0] + ra[c]
        near_right(c, 0).start()
        far_left(c).wait_recv()
        acc[c, c_left, core, 1] = acc[c, c_left, core, 1] + rb[c]
        near_left(c, 1).start()

    def stage4(c):
        remote(rl.at[c], rl.at[c], rs_send.at[3], rs_recv.at[3, c], right).wait_recv()
        remote(rr.at[c], rr.at[c], rs_send.at[4], rs_recv.at[4, c], left).wait_recv()
        for j in range(2):
            y_ref[:, pl.ds(pl.multiple_of(c * COLS + j * half, half), half)] = (acc[c, chip, core, j] + rl[c, j] + rr[c, j]).astype(BF16)

    per = wide // COLS

    def down_item(c, e):
        return n_gate + (c // per) * n_exp + e

    def down(c):
        @pl.when(c % per == 0)
        def _():
            for e in range(n_exp):
                wait_slot(down_item(c, e) % SLOTS)
        for e in range(n_exp):
            slot = down_item(c, e) % SLOTS
            parts = [jnp.dot(hid[e, :, j * kw:(j + 1) * kw],
                             ring[slot, :, pl.ds(pl.multiple_of(j * wide + (c % per) * COLS, COLS), COLS)], preferred_element_type=F32)
                     for j in range(2)]
            outs[e] = (parts[0] + parts[1]).astype(BF16)

    def put_back(c):
        for ch in range(chips):
            total = None
            for e in range(n_exp):
                put = jnp.dot(smat[e, ch * lanes:(ch + 1) * lanes, :], outs[e, (ch // 2) * half_slot:(ch // 2 + 1) * half_slot, :],
                              preferred_element_type=F32)
                gate = gmat[e, ch * lanes:(ch + 1) * lanes, :]
                put = put * jnp.concatenate([gate] * (COLS // lanes), axis=1)
                total = put if total is None else total + put
            for j in range(2):
                acc[c, ch, :, j] = total[:, j * half:(j + 1) * half].reshape(2, tok_dev, half)

        @pl.when(c % per == per - 1)
        def _():
            for e in range(n_exp):
                nxt = down_item(c, e) + SLOTS

                @pl.when(nxt < n_items)
                def _():
                    start_down(nxt)

    def chunk_body(c, carry):
        down(c)

        @pl.when(c >= 1)
        def _():
            stage2(c - 1)
        put_back(c)
        to_sibling(c).start()

        @pl.when(c >= 2)
        def _():
            stage3(c - 2)

        @pl.when(c >= 4)
        def _():
            stage4(c - 4)
        return carry

    lax.fori_loop(0, n_chunks, chunk_body, 0)
    last = n_chunks - 1
    stage2(last)
    stage3(last - 1)
    stage4(last - 3)
    stage3(last)
    for c in range(last - 2, n_chunks):
        stage4(c)

    for i in range(2):
        table_all(i).wait_send()
    everything = xbuf.at[:, pl.ds(0, (2 * chips - 1) * tok_dev), :]
    remote(everything, everything, ag_send, ag_recv.at[0, 0], sibling).wait_send()
    for i, ref in enumerate((sib, ra, rb, rl, rr)):
        remote(ref, ref, rs_send.at[i], rs_recv.at[i, 0], sibling).wait_send()


def solution(mesh):
    n = mesh.shape["ep"]
    row_spec = P(("dp", "ep"))
    expert_spec = P("ep")

    def local_step(tok, route, gate, wg, wu, wd):
        tok_dev, d_model = tok.shape
        n_exp, _, d_ff = wg.shape
        top_k = route.shape[1]
        cap = tok_dev // 2
        chips = n // 2
        lanes = 2 * tok_dev
        kw = d_model // KCHUNKS
        n_chunks = d_model // COLS
        dims = (n, tok_dev, d_model, d_ff, n_exp, top_k, cap)

        hbm = pl.BlockSpec(memory_space=pl.ANY)
        vmem = pl.BlockSpec(memory_space=pltpu.VMEM)
        return pl.pallas_call(
            functools.partial(moe_kernel, dims),
            out_shape=pltpu.VMEM((tok_dev, d_model), BF16),
            in_specs=[hbm, vmem, vmem, hbm, hbm, hbm],
            out_specs=vmem,
            scratch_shapes=[
                pltpu.VMEM((KCHUNKS, n * tok_dev, kw), BF16),
                pltpu.VMEM((2 * top_k, lanes), F32),
                pltpu.VMEM((n, 2 * top_k, lanes), F32),
                pltpu.VMEM((chips, 2 * n_exp, lanes), F32),
                pltpu.VMEM((2, n_exp, n * cap // 2, n * tok_dev // 2), BF16),
                pltpu.VMEM((n_exp, n * tok_dev, n * cap // 2), BF16),
                pltpu.VMEM((n_exp, n * tok_dev, lanes), F32),
                pltpu.VMEM((2, n_exp, 2, n * cap // 2, kw), BF16),
                pltpu.VMEM((n_exp, n * cap, d_ff), F32),
                pltpu.VMEM((n_exp, n * cap, d_ff), F32),
                pltpu.VMEM((n_exp, n * cap, d_ff), BF16),
                pltpu.VMEM((SLOTS, kw, d_ff), BF16),
                pltpu.VMEM((n_exp, n * cap, COLS), BF16),
                pltpu.VMEM((n_chunks, chips, 2, 2, tok_dev, COLS // 2), F32),
                pltpu.VMEM((n_chunks, chips, 2, tok_dev, COLS // 2), F32),
                pltpu.VMEM((n_chunks, tok_dev, COLS // 2), F32),
                pltpu.VMEM((n_chunks, tok_dev, COLS // 2), F32),
                pltpu.VMEM((n_chunks, 2, tok_dev, COLS // 2), F32),
                pltpu.VMEM((n_chunks, 2, tok_dev, COLS // 2), F32),
                pltpu.SemaphoreType.DMA((KCHUNKS,)),
                pltpu.SemaphoreType.DMA((2,)),
                pltpu.SemaphoreType.DMA((2,)),
                pltpu.SemaphoreType.DMA,
                pltpu.SemaphoreType.DMA((KCHUNKS, 2)),
                pltpu.SemaphoreType.DMA((SLOTS,)),
                pltpu.SemaphoreType.DMA((5,)),
                pltpu.SemaphoreType.DMA((5, n_chunks)),
            ],
            compiler_params=pltpu.CompilerParams(collective_id=0, has_side_effects=True, vmem_limit_bytes=66_700_000),
        )(tok, route.T, gate.T, wg, wu, wd)

    return jax.shard_map(local_step, mesh=mesh, in_specs=(row_spec, row_spec, row_spec, expert_spec, expert_spec, expert_spec), out_specs=row_spec, check_vma=False)
```

```python
import functools

import jax
import jax.numpy as jnp
from jax import lax
from jax.experimental import pallas as pl
from jax.experimental.pallas import tpu as pltpu
from jax.sharding import PartitionSpec as P

F32 = jnp.float32
BF16 = jnp.bfloat16
KCHUNKS = 4
COLS = 256
SLOTS = 22
FILL = (4, 8, SLOTS // 2)


def moe_kernel(dims, x_hbm, route_ref, gate_ref, wg_hbm, wu_hbm, wd_hbm, y_ref,
               xbuf, comb_in, comb, codes, pmat, smat, gmat, xs, gacc, uacc, hid, ring, outs, acc, sib, ra, rb, rl, rr,
               x_sem, comb_send, comb_recv, ag_send, ag_recv, w_sem, rs_send, rs_recv):
    n, tok_dev, d_model, d_ff, n_exp, top_k, cap = dims
    chips = n // 2
    lanes = 2 * tok_dev
    kw = d_model // KCHUNKS
    n_steps = KCHUNKS * n_exp
    single = 2 * n_exp
    n_gate = 2 * n_steps
    wide = d_ff // 2
    n_items = n_gate + n_exp * (d_model // wide)
    n_chunks = d_model // COLS
    half_tok = n * tok_dev // 2
    half_slot = n * cap // 2

    me = lax.axis_index("ep")
    chip, core = me // 2, me % 2
    other = 1 - core
    sibling = chip * 2 + other
    c_right, c_left, c_opp = (chip + 1) % chips, (chip + chips - 1) % chips, (chip + 2) % chips
    right, left, opp = c_right * 2 + core, c_left * 2 + core, c_opp * 2 + core

    def remote(src, dst, send, recv, dev):
        return pltpu.make_async_remote_copy(src_ref=src, dst_ref=dst, send_sem=send, recv_sem=recv,
                                            device_id={"ep": dev}, device_id_type=pl.DeviceIdType.MESH)

    def x_copy(kc):
        return pltpu.make_async_copy(x_hbm.at[:, pl.ds(kc * kw, kw)],
                                     xbuf.at[kc, pl.ds(pl.multiple_of(me * tok_dev, tok_dev), tok_dev), :], x_sem.at[kc])

    def gate_copy(w, kc, e, slot):
        return pltpu.make_async_copy(w.at[e, pl.ds(pl.multiple_of(kc * kw, kw), kw), :], ring.at[slot], w_sem.at[slot])

    def wait_slot(slot):
        gate_copy(wg_hbm, 0, 0, slot).wait()

    def start_pair(kc, e, item):
        gate_copy(wg_hbm, kc, e, item % SLOTS).start()
        gate_copy(wu_hbm, kc, e, (item + 1) % SLOTS).start()

    def start_down(item):
        c, e, slot = (item - n_gate) // n_exp, (item - n_gate) % n_exp, item % SLOTS
        cols = pl.ds(pl.multiple_of(c * wide, wide), wide)
        for j in range(2):
            pltpu.make_async_copy(wd_hbm.at[e, pl.ds(j * kw, kw), cols], ring.at[slot, :, pl.ds(j * wide, wide)], w_sem.at[slot]).start()

    def start_step(step):
        @pl.when(step < single)
        def _():
            start_pair(step // n_exp, step % n_exp, 2 * step)

        @pl.when((step >= single) & (step < n_steps))
        def _():
            start_pair(2 + step % 2, (step - single) // 2, 2 * step)

        @pl.when((step >= n_steps) & (2 * step < n_items))
        def _():
            start_down(2 * step)
            start_down(2 * step + 1)

    def fill(part):
        for step in range(FILL[part - 1] if part else 0, FILL[part]):
            start_pair(step // n_exp, step % n_exp, 2 * step)

    for kc in range(KCHUNKS):
        x_copy(kc).start()
    fill(0)

    mine = lax.broadcasted_iota(jnp.int32, (top_k, lanes), 1) // tok_dev == core
    for i, part in enumerate((route_ref[...].astype(F32), gate_ref[...])):
        comb_in[i * top_k:(i + 1) * top_k, :] = jnp.where(mine, jnp.concatenate([part, part], axis=1), 0.0)

    barrier = pltpu.get_barrier_semaphore()
    for off in range(1, n):
        pl.semaphore_signal(barrier, inc=1, device_id={"ep": (me + off) % n}, device_id_type=pl.DeviceIdType.MESH)
    pl.semaphore_wait(barrier, n - 1)

    def blocks(kc, first, count=1):
        return xbuf.at[kc, pl.ds(pl.multiple_of(first * tok_dev, tok_dev), count * tok_dev), :]

    def ag_copy(kc, src, dev, over_chip):
        return remote(blocks(kc, src), blocks(kc, src), ag_send, ag_recv.at[kc, over_chip], dev)

    def send_own(kc):
        for dev in (right, left, opp):
            ag_copy(kc, me, dev, 0).start()
        ag_copy(kc, me, sibling, 1).start()

    def forward(kc):
        remote(blocks(kc, 0, chips - 1), blocks(kc, 0, chips - 1), ag_send, ag_recv.at[kc, 0], sibling).wait_recv()
        for src in (left, right, opp):
            ag_copy(kc, src, sibling, 1).start()

    def gathered(kc):
        remote(blocks(kc, 0, chips), blocks(kc, 0, chips), ag_send, ag_recv.at[kc, 1], sibling).wait_recv()

    def table_copy(i, dev):
        rows = pl.ds(i * top_k, top_k)
        return remote(comb_in.at[rows, :], comb.at[me, rows, :], comb_send.at[i], comb_recv.at[i], dev)

    def table_all(i):
        part = comb.at[pl.ds(0, n - 1), pl.ds(i * top_k, top_k), :]
        return remote(part, part, comb_send.at[i], comb_recv.at[i], sibling)

    for off in range(1, n):
        table_copy(0, (me + off) % n).start()
    comb[me] = comb_in[...]
    x_copy(0).wait()
    send_own(0)
    for off in range(1, n):
        table_copy(1, (me + off) % n).start()
    for kc in range(1, KCHUNKS):
        x_copy(kc).wait()
        send_own(kc)
    fill(1)
    table_all(0).wait_recv()

    t_row = lax.broadcasted_iota(jnp.int32, (lanes, lanes), 0)
    t_col = lax.broadcasted_iota(jnp.int32, (lanes, lanes), 1)
    before = jnp.where((t_row < t_col) & (t_row // tok_dev == t_col // tok_dev), 1.0, 0.0).astype(BF16)
    e_id = (lax.broadcasted_iota(jnp.int32, (n_exp, lanes), 0) + me * n_exp).astype(F32)
    lane_base = ((lax.broadcasted_iota(jnp.int32, (n_exp, lanes), 1) // tok_dev) * cap).astype(F32)
    for c in range(chips):
        route = comb[2 * c, 0:top_k] + comb[2 * c + 1, 0:top_k]
        hits = jnp.zeros((n_exp, lanes), F32)
        for k in range(top_k):
            hits = hits + jnp.where(jnp.broadcast_to(route[k:k + 1, :], (n_exp, lanes)) == e_id, 1.0, 0.0)
        rank = jnp.dot(hits.astype(BF16), before, preferred_element_type=F32)
        codes[c, 0:n_exp, :] = jnp.where(hits > 0.0, rank + lane_base + float((c % 2) * 2 * cap), -1.0)

    def gate_codes():
        table_all(1).wait_recv()
        for c in range(chips):
            both = comb[2 * c] + comb[2 * c + 1]
            gates = jnp.zeros((n_exp, lanes), F32)
            for k in range(top_k):
                same = jnp.broadcast_to(both[k:k + 1, :], (n_exp, lanes)) == e_id
                gates = gates + jnp.where(same, jnp.broadcast_to(both[top_k + k:top_k + k + 1, :], (n_exp, lanes)), 0.0)
            codes[c, n_exp:2 * n_exp, :] = gates

    def gather_tables(e, carry):
        slot_row = lax.broadcasted_iota(jnp.int32, (half_slot, lanes), 0).astype(F32)
        for c in range(chips):
            code = jnp.broadcast_to(codes[c, pl.ds(e, 1), :], (half_slot, lanes))
            pmat[c // 2, e, :, (c % 2) * lanes:(c % 2 + 1) * lanes] = jnp.where(code == slot_row, 1.0, 0.0).astype(BF16)
        return carry

    def scatter_tables(e):
        slot_col = lax.broadcasted_iota(jnp.int32, (lanes, half_slot), 1).astype(F32)
        for c in range(chips):
            code = jnp.broadcast_to(codes[c, pl.ds(e, 1), :], (half_slot, lanes))
            smat[e, c * lanes:(c + 1) * lanes, :] = jnp.where(code.T == slot_col, 1.0, 0.0).astype(BF16)
            gate = jnp.broadcast_to(codes[c, pl.ds(n_exp + e, 1), :], (lanes, lanes))
            gmat[e, c * lanes:(c + 1) * lanes, :] = gate.T

    lax.fori_loop(0, n_exp, gather_tables, 0)
    forward(0)
    fill(2)
    gate_codes()

    def gather(kc, g):
        gathered(kc)
        for h in range(2):
            picks = pmat[h].reshape(n_exp * half_slot, half_tok)
            for at in range(0, kw, 256):
                rows = jnp.dot(picks, xbuf[kc, h * half_tok:(h + 1) * half_tok, at:at + 256], preferred_element_type=F32)
                xs[g, :, h, :, at:at + 256] = rows.astype(BF16).reshape(n_exp, half_slot, 256)

    def expert_pass(e, slots, groups, first, last):
        for at in range(0, d_ff, 256):
            cols = slice(at, at + 256)
            g = u = None
            for i in range(groups):
                rows = xs[i, e].reshape(2 * half_slot, kw)
                dg = jnp.dot(rows, ring[slots[2 * i], :, cols], preferred_element_type=F32)
                du = jnp.dot(rows, ring[slots[2 * i + 1], :, cols], preferred_element_type=F32)
                g, u = (dg, du) if g is None else (g + dg, u + du)
            if not first:
                g = gacc[e, :, cols] + g
                u = uacc[e, :, cols] + u
            if last:
                hid[e, :, cols] = (jax.nn.silu(g) * u).astype(BF16)
            else:
                gacc[e, :, cols] = g
                uacc[e, :, cols] = u

    def take(step, count):
        slots = [(2 * step + i) % SLOTS for i in range(2 * count)]
        for slot in slots:
            wait_slot(slot)
        return slots

    def refill(step, count):
        for i in range(count):
            start_step(step + i + SLOTS // 2)

    for kc in range(2):
        def pair_body(i, carry, kc=kc):
            step = kc * n_exp + 2 * i
            slots = take(step, 2)
            for j in range(2):
                if kc == 0:
                    scatter_tables(2 * i + j)
                expert_pass(2 * i + j, slots[2 * j:2 * j + 2], 1, kc == 0, False)
            refill(step, 2)
            if kc == 0:
                @pl.when(i == n_exp // 2 - 2)
                def _():
                    forward(1)
            else:
                @pl.when(i == 0)
                def _():
                    forward(2)

                @pl.when(i == n_exp // 2 - 2)
                def _():
                    forward(3)
            return carry

        gather(kc, 0)
        lax.fori_loop(0, n_exp // 2, pair_body, 0)

    def last_body(i, carry):
        step = single + 4 * i
        slots = take(step, 4)
        for j in range(2):
            expert_pass(2 * i + j, slots[4 * j:4 * j + 4], 2, False, True)
        refill(step, 4)
        return carry

    gather(2, 0)
    gather(3, 1)
    lax.fori_loop(0, n_exp // 2, last_body, 0)

    half = COLS // 2

    def to_sibling(c):
        return remote(acc.at[c, :, other], sib.at[c], rs_send.at[0], rs_recv.at[0, c], sibling)

    def far_right(c):
        return remote(acc.at[c, c_opp, core, 0], ra.at[c], rs_send.at[1], rs_recv.at[1, c], right)

    def far_left(c):
        return remote(acc.at[c, c_opp, core, 1], rb.at[c], rs_send.at[2], rs_recv.at[2, c], left)

    def near_right(c, j):
        return remote(acc.at[c, c_right, core, j], rl.at[c, j], rs_send.at[3], rs_recv.at[3, c], right)

    def near_left(c, j):
        return remote(acc.at[c, c_left, core, j], rr.at[c, j], rs_send.at[4], rs_recv.at[4, c], left)

    def stage2(c):
        to_sibling(c).wait_recv()
        acc[c, c_opp, core] = acc[c, c_opp, core] + sib[c, c_opp]
        far_right(c).start()
        far_left(c).start()
        acc[c, c_right, core] = acc[c, c_right, core] + sib[c, c_right]
        near_right(c, 1).start()
        acc[c, c_left, core] = acc[c, c_left, core] + sib[c, c_left]
        near_left(c, 0).start()

    def stage3(c):
        far_right(c).wait_recv()
        acc[c, c_right, core, 0] = acc[c, c_right, core, 0] + ra[c]
        near_right(c, 0).start()
        far_left(c).wait_recv()
        acc[c, c_left, core, 1] = acc[c, c_left, core, 1] + rb[c]
        near_left(c, 1).start()

    def stage4(c):
        remote(rl.at[c], rl.at[c], rs_send.at[3], rs_recv.at[3, c], right).wait_recv()
        remote(rr.at[c], rr.at[c], rs_send.at[4], rs_recv.at[4, c], left).wait_recv()
        for j in range(2):
            y_ref[:, pl.ds(pl.multiple_of(c * COLS + j * half, half), half)] = (acc[c, chip, core, j] + sib[c, chip, j] + rl[c, j] + rr[c, j]).astype(BF16)

    per = wide // COLS

    def down_item(c, e):
        return n_gate + (c // per) * n_exp + e

    def down(c):
        @pl.when(c % per == 0)
        def _():
            for e in range(n_exp):
                wait_slot(down_item(c, e) % SLOTS)
        for e in range(n_exp):
            slot = down_item(c, e) % SLOTS
            for r in range(2):
                rows = slice(r * half_slot, (r + 1) * half_slot)
                parts = [jnp.dot(hid[e, rows, j * kw:(j + 1) * kw],
                                 ring[slot, :, pl.ds(pl.multiple_of(j * wide + (c % per) * COLS, COLS), COLS)], preferred_element_type=F32)
                         for j in range(2)]
                outs[e, rows, :] = (parts[0] + parts[1]).astype(BF16)

    def put_back(c):
        for ch in range(chips):
            total = None
            for e in range(n_exp):
                put = jnp.dot(smat[e, ch * lanes:(ch + 1) * lanes, :], outs[e, (ch // 2) * half_slot:(ch // 2 + 1) * half_slot, :],
                              preferred_element_type=F32)
                gate = gmat[e, ch * lanes:(ch + 1) * lanes, :]
                put = put * jnp.concatenate([gate] * (COLS // lanes), axis=1)
                total = put if total is None else total + put
            for j in range(2):
                acc[c, ch, :, j] = total[:, j * half:(j + 1) * half].reshape(2, tok_dev, half)

    def refill_down(c):
        @pl.when(c % per == per - 1)
        def _():
            for e in range(n_exp):
                nxt = down_item(c, e) + SLOTS

                @pl.when(nxt < n_items)
                def _():
                    start_down(nxt)

    def chunk_body(c, carry):
        down(c)

        @pl.when(c >= 1)
        def _():
            stage2(c - 1)
        put_back(c)
        to_sibling(c).start()
        refill_down(c)

        @pl.when(c >= 2)
        def _():
            stage3(c - 2)

        return carry

    lax.fori_loop(0, n_chunks, chunk_body, 0)
    last = n_chunks - 1
    stage2(last)
    stage3(last - 1)
    for c in range(last - 2):
        stage4(c)
    stage3(last)
    for c in range(last - 2, n_chunks):
        stage4(c)

    for i in range(2):
        table_all(i).wait_send()
    everything = xbuf.at[:, pl.ds(0, (2 * chips - 1) * tok_dev), :]
    remote(everything, everything, ag_send, ag_recv.at[0, 0], sibling).wait_send()
    for i, ref in enumerate((sib, ra, rb, rl, rr)):
        remote(ref, ref, rs_send.at[i], rs_recv.at[i, 0], sibling).wait_send()


def solution(mesh):
    n = mesh.shape["ep"]
    row_spec = P(("dp", "ep"))
    expert_spec = P("ep")

    def local_step(tok, route, gate, wg, wu, wd):
        tok_dev, d_model = tok.shape
        n_exp, _, d_ff = wg.shape
        top_k = route.shape[1]
        cap = tok_dev // 2
        chips = n // 2
        lanes = 2 * tok_dev
        kw = d_model // KCHUNKS
        n_chunks = d_model // COLS
        dims = (n, tok_dev, d_model, d_ff, n_exp, top_k, cap)

        hbm = pl.BlockSpec(memory_space=pl.ANY)
        vmem = pl.BlockSpec(memory_space=pltpu.VMEM)
        return pl.pallas_call(
            functools.partial(moe_kernel, dims),
            out_shape=pltpu.VMEM((tok_dev, d_model), BF16),
            in_specs=[hbm, vmem, vmem, hbm, hbm, hbm],
            out_specs=vmem,
            scratch_shapes=[
                pltpu.VMEM((KCHUNKS, n * tok_dev, kw), BF16),
                pltpu.VMEM((2 * top_k, lanes), F32),
                pltpu.VMEM((n, 2 * top_k, lanes), F32),
                pltpu.VMEM((chips, 2 * n_exp, lanes), F32),
                pltpu.VMEM((2, n_exp, n * cap // 2, n * tok_dev // 2), BF16),
                pltpu.VMEM((n_exp, n * tok_dev, n * cap // 2), BF16),
                pltpu.VMEM((n_exp, n * tok_dev, lanes), F32),
                pltpu.VMEM((2, n_exp, 2, n * cap // 2, kw), BF16),
                pltpu.VMEM((n_exp, n * cap, d_ff), F32),
                pltpu.VMEM((n_exp, n * cap, d_ff), F32),
                pltpu.VMEM((n_exp, n * cap, d_ff), BF16),
                pltpu.VMEM((SLOTS, kw, d_ff), BF16),
                pltpu.VMEM((n_exp, n * cap, COLS), BF16),
                pltpu.VMEM((n_chunks, chips, 2, 2, tok_dev, COLS // 2), F32),
                pltpu.VMEM((n_chunks, chips, 2, tok_dev, COLS // 2), F32),
                pltpu.VMEM((n_chunks, tok_dev, COLS // 2), F32),
                pltpu.VMEM((n_chunks, tok_dev, COLS // 2), F32),
                pltpu.VMEM((n_chunks, 2, tok_dev, COLS // 2), F32),
                pltpu.VMEM((n_chunks, 2, tok_dev, COLS // 2), F32),
                pltpu.SemaphoreType.DMA((KCHUNKS,)),
                pltpu.SemaphoreType.DMA((2,)),
                pltpu.SemaphoreType.DMA((2,)),
                pltpu.SemaphoreType.DMA,
                pltpu.SemaphoreType.DMA((KCHUNKS, 2)),
                pltpu.SemaphoreType.DMA((SLOTS,)),
                pltpu.SemaphoreType.DMA((5,)),
                pltpu.SemaphoreType.DMA((5, n_chunks)),
            ],
            compiler_params=pltpu.CompilerParams(collective_id=0, has_side_effects=True, vmem_limit_bytes=66_700_000),
        )(tok, route.T, gate.T, wg, wu, wd)

    return jax.shard_map(local_step, mesh=mesh, in_specs=(row_spec, row_spec, row_spec, expert_spec, expert_spec, expert_spec), out_specs=row_spec, check_vma=False)
```
